32 devices in a mesh: req: 2 (over core), seq: 16 (over z, y, x).
Axes of the slice: x: 2, y: 2, z: 4, core: 2. Of those that a mesh axis runs over, the one named last changes fastest.
Arguments:
- image_query: bfloat16 [256, 1536], P(('req', 'seq')), parts along dimension 0, may hold values from -6 to 6
- image_key: bfloat16 [256, 1536], P(('req', 'seq')), parts along dimension 0, may hold values from -6 to 6
- image_value: bfloat16 [256, 1536], P(('req', 'seq')), parts along dimension 0, may hold values from -6 to 6
- text_query: bfloat16 [1024, 1536], P('req'), parts along dimension 0, may hold values from -6 to 6
- text_key: bfloat16 [1024, 1536], P('req'), parts along dimension 0, may hold values from -6 to 6
- text_value: bfloat16 [1024, 1536], P('req'), parts along dimension 0, may hold values from -6 to 6
- image_query_gain: float32 [128], replicated, may hold values from 1 to 8
- image_key_gain: float32 [128], replicated, may hold values from 1 to 8
- text_query_gain: float32 [128], replicated, may hold values from 1 to 2.5
- text_key_gain: float32 [128], replicated, may hold values from 1 to 2.5
- image_order: int32 [256], P(('req', 'seq')), parts along dimension 0, may hold values from 0 to 127, each once
- text_length: int32 [2], P('req'), parts along dimension 0, may hold values from 256 to 512
Outputs:
- image_out: bfloat16 [256, 1536], P(('req', 'seq')), parts along dimension 0
- text_out: bfloat16 [1024, 1536], P(('req', 'seq')), parts along dimension 0
The draws below stay inside these ranges and needn't reach their ends.
There are 2 independent parts, one for each index of `req`. The reference program is written for one: setup_inputs(seed, part) draws one part's arguments, and reference() takes and returns one part's arrays. A program takes and returns all parts, laid end to end along the dimension named above; an argument that names none is the same for every part. Nothing has to cross between parts.
Inputs may be any that keep to these rules, and one draw needn't show every extreme that they name: `image_order`: every position 0 to 127 appears once.
All inputs are finite; a program needn't handle non-finite values.
Results may differ from the reference program's by a relative error of at most 0.005.
The reference program's roundings to bfloat16 on the way (of `weights`) count: a program that leaves them out, or rounds other values in their place, can miss the bound.
Values may be sent and summed in bfloat16 or wider, within the bound.
A program may use at most 64 MiB of HBM per device.

```python
import jax
import jax.numpy as jnp
from jax import lax

H = 12
HD = 128
TXT = 512
GRID_W = 64
TOK_DEV = 8
IMG = 128
N_SEQ = 16


def draw_image_query(key, part):
    queries = jax.random.normal(jax.random.fold_in(key, 1), (IMG, H * HD), jnp.float32)
    return jnp.clip(queries, -6.0, 6.0).astype(jnp.bfloat16)


def draw_image_key(key, part):
    keys_drawn = jax.random.normal(jax.random.fold_in(key, 2), (IMG, H * HD), jnp.float32)
    return jnp.clip(keys_drawn, -6.0, 6.0).astype(jnp.bfloat16)


def draw_image_query_gain(key, part):
    return jax.random.uniform(jax.random.fold_in(key, 5), (HD,), jnp.float32, 1.0, 2.5)


def draw_image_key_gain(key, part):
    return jax.random.uniform(jax.random.fold_in(key, 6), (HD,), jnp.float32, 1.0, 2.5)


def level_of(own_key, dims, cuts, low, top_value):
    level, own = 1.0, jax.random.fold_in(own_key, 6)
    for dim, parts in cuts:
        heights = jnp.exp(jax.random.uniform(jax.random.fold_in(own, dim), (parts,), jnp.float32, low / len(cuts), top_value / len(cuts)))
        level = level * jnp.repeat(heights, dims[dim] // parts).reshape([-1 if axis == dim else 1 for axis in range(len(dims))])
    return level


def bell_draw(stream_key, dims, deviation, limit, pieces=(), held_as=jnp.bfloat16):
    level = level_of(stream_key, dims, pieces, -0.22, 0.18) if pieces else 1.0
    values = jax.random.normal(stream_key, dims, jnp.float32) * deviation * level
    return jnp.minimum(jnp.maximum(values, -limit), limit).astype(held_as)


def setup_inputs(seed: int = 0, part: int = 0) -> dict:
    key_of = jax.random.split(jax.random.key(seed), 13)
    part_keys = jax.random.split(jax.random.fold_in(key_of[12], part), 13)
    image_query = draw_image_query(jax.random.fold_in(jax.random.fold_in(key_of[12], part), 71), part)
    image_key = draw_image_key(jax.random.fold_in(jax.random.fold_in(key_of[12], part), 71), part)
    image_value = bell_draw(part_keys[2], (IMG, H * HD), 1.0, 6.0, ((0, 16),))
    text_query = bell_draw(part_keys[3], (TXT, H * HD), 1.0, 6.0)
    text_key = bell_draw(part_keys[4], (TXT, H * HD), 1.0, 6.0)
    text_value = bell_draw(part_keys[5], (TXT, H * HD), 1.0, 6.0)
    image_query_gain = draw_image_query_gain(jax.random.fold_in(key_of[12], 71), part)
    image_key_gain = draw_image_key_gain(jax.random.fold_in(key_of[12], 71), part)
    text_query_gain = jnp.clip(jax.random.uniform(key_of[8], (HD,), jnp.float32, 1.0, 2.5), 1.0, 2.5)
    text_key_gain = jnp.clip(jax.random.uniform(key_of[9], (HD,), jnp.float32, 1.0, 2.5), 1.0, 2.5)
    image_order = jax.random.permutation(part_keys[10], IMG).astype(jnp.int32)
    text_length = jax.random.randint(part_keys[11], (1,), TXT // 2, TXT + 1).astype(jnp.int32)
    return {"image_query": image_query, "image_key": image_key, "image_value": image_value, "text_query": text_query, "text_key": text_key, "text_value": text_value, "image_query_gain": image_query_gain, "image_key_gain": image_key_gain, "text_query_gain": text_query_gain, "text_key_gain": text_key_gain, "image_order": image_order, "text_length": text_length}


epsilon = 1e-06
masked_score = -1e+30

def head_norm(values, norm_gain, head_count):
    row_count = values.shape[0]
    shaped = values.astype(jnp.float32).reshape(row_count, head_count, -1)
    mean_square = lax.optimization_barrier(jnp.mean(shaped * shaped, axis=-1, keepdims=True))
    return shaped * lax.rsqrt(mean_square + epsilon) * norm_gain

def rotate(normed, positions, half_length):
    row_count, head_count, head_dim = normed.shape
    pair_count = head_dim // 2
    pair_ids = jnp.arange(pair_count)
    first_axis = pair_ids < 8
    second = pair_ids < 36
    within = jnp.where(first_axis, pair_ids, jnp.where(second, pair_ids - 8, pair_ids - 36)).astype(jnp.float32)
    axis_dim = jnp.where(first_axis, 16.0, 56.0).astype(jnp.float32)
    frequency = jnp.power(jnp.float32(10000.0), -2.0 * within / axis_dim)
    image_index = positions // half_length
    inside = positions % half_length
    row_place = inside // GRID_W
    column_place = inside % GRID_W
    coordinate = jnp.where(first_axis[None, :], image_index[:, None], jnp.where(second[None, :], row_place[:, None], column_place[:, None])).astype(jnp.float32)
    angles = coordinate * frequency[None, :]
    cosine = jnp.cos(angles)[:, None, :]
    sine_part = jnp.sin(angles)[:, None, :]
    paired = normed.reshape(row_count, head_count, pair_count, 2)
    even_part = paired[..., 0]
    odd_part = paired[..., 1]
    turned = jnp.stack([even_part * cosine - odd_part * sine_part, even_part * sine_part + odd_part * cosine], axis=-1)
    return turned.reshape(row_count, head_count * head_dim)

def reference(image_query, image_key, image_value, text_query, text_key, text_value, image_query_gain, image_key_gain, text_query_gain, text_key_gain, image_order, text_length):
    head_count = image_query.shape[1] // HD
    half_length = IMG // 2
    query_img = lax.optimization_barrier(rotate(head_norm(image_query, image_query_gain, head_count), image_order, half_length).astype(jnp.bfloat16))
    key_img = lax.optimization_barrier(rotate(head_norm(image_key, image_key_gain, head_count), image_order, half_length).astype(jnp.bfloat16))
    query_txt = lax.optimization_barrier(head_norm(text_query, text_query_gain, head_count).reshape(TXT, -1).astype(jnp.bfloat16))
    key_txt = lax.optimization_barrier(head_norm(text_key, text_key_gain, head_count).reshape(TXT, -1).astype(jnp.bfloat16))
    all_keys = jnp.concatenate([key_txt, key_img], axis=0).astype(jnp.float32)
    all_values = jnp.concatenate([text_value, image_value], axis=0).astype(jnp.float32)
    key_count = all_keys.shape[0]
    key_heads = all_keys.reshape(key_count, head_count, HD)
    value_heads = all_values.reshape(key_count, head_count, HD)
    valid = jnp.concatenate([jnp.arange(TXT) < text_length[0], jnp.ones((IMG,), dtype=bool)])
    scaling = HD ** (-0.5)

    def attend(block):
        row_count = block.shape[0]
        query_heads = block.astype(jnp.float32).reshape(row_count, head_count, HD)
        scores = jnp.einsum('rhd,shd->rhs', query_heads, key_heads) * scaling
        scores = jnp.where(valid[None, None, :], scores, masked_score)
        row_max = lax.optimization_barrier(jnp.max(scores, axis=-1))
        expo = jnp.exp(scores - row_max[..., None])
        expo = jnp.where(valid[None, None, :], expo, 0.0)
        totals = lax.optimization_barrier(jnp.sum(expo, axis=-1))
        weights = lax.optimization_barrier(expo.astype(jnp.bfloat16)).astype(jnp.float32)
        blended = jnp.einsum('rhs,shd->rhd', weights, value_heads)
        return (blended / totals[..., None]).reshape(row_count, -1).astype(jnp.bfloat16)
    text_out = lax.map(attend, query_txt.reshape(N_SEQ, TXT // N_SEQ, -1)).reshape(TXT, -1)
    image_out = lax.map(attend, query_img.reshape(N_SEQ, TOK_DEV, -1)).reshape(IMG, -1)
    return (image_out, text_out)
```

```python
import functools
import math

import jax
import jax.numpy as jnp
from jax import lax
from jax.experimental import pallas as pl
from jax.experimental.pallas import tpu as pltpu
from jax.sharding import PartitionSpec as P

GRID_W = 64
EPS = 1e-06
LOW = -1e30
TEAM = 4
MESH = pl.DeviceIdType.MESH


def rsqrt_mean(values):
    return lax.rsqrt(jnp.mean(values * values, axis=-1, keepdims=True) + EPS)


def kernel(
    devices,
    iq_ref,
    ik_ref,
    iv_ref,
    tq_ref,
    tk_ref,
    tv_ref,
    iqg_ref,
    ikg_ref,
    tqg_ref,
    tkg_ref,
    order_ref,
    length_ref,
    out_ref,
    iq_buf,
    ik_buf,
    iv_buf,
    tq_buf,
    tk_buf,
    tv_buf,
    gain_buf,
    order_buf,
    length_buf,
    kv_own,
    q_own,
    kv_all,
    q_team,
    qs,
    m_buf,
    l_buf,
    o_buf,
    back_own,
    back_all,
    local_sem,
    kv_send,
    kv_recv,
    q_send,
    q_recv,
    back_send,
    back_recv,
):
    me = lax.axis_index("seq")
    req = lax.axis_index("req")
    seat = me % TEAM
    team = me // TEAM
    mates = [(team * TEAM + (seat ^ k), seat ^ k) for k in (3, 2, 1)]

    barrier = pltpu.get_barrier_semaphore()
    for d in range(1, devices):
        pl.semaphore_signal(
            barrier, inc=1, device_id=(req, (me + d) % devices), device_id_type=MESH
        )

    own_rows, width = iq_buf.shape
    size = gain_buf.shape[-1]
    heads = width // size
    text_rows, span = tk_buf.shape
    per = span // size
    team_text = tq_buf.shape[0]
    share = team_text // TEAM
    team_rows = team_text + TEAM * own_rows
    scale = math.log2(math.e) / math.sqrt(size)

    lanes = pl.ds(pl.multiple_of(seat * span, span), span)
    text = pl.ds(pl.multiple_of(team * team_text, team_text), team_text)
    loads = []
    for src, dst in (
        (order_ref, order_buf),
        (ik_ref, ik_buf),
        (ikg_ref, gain_buf.at[0]),
        (iv_ref, iv_buf),
        (iq_ref, iq_buf),
        (iqg_ref, gain_buf.at[1]),
        (tk_ref.at[:, lanes], tk_buf),
        (tkg_ref, gain_buf.at[2]),
        (tq_ref.at[text, lanes], tq_buf),
        (tqg_ref, gain_buf.at[3]),
        (length_ref, length_buf),
        (tv_ref.at[:, lanes], tv_buf),
    ):
        copy = pltpu.make_async_copy(src, dst, local_sem.at[len(loads)])
        copy.start()
        loads.append(copy)

    loads[0].wait()
    half_length = own_rows * devices // 2
    lane = lax.broadcasted_iota(jnp.int32, (own_rows, size), 1)
    row = lax.broadcasted_iota(jnp.int32, (own_rows, size), 0)
    pair_id = lane // 2
    first = pair_id < 8
    second = pair_id < 36
    coordinate = jnp.zeros((own_rows, size), jnp.int32)
    for r in range(own_rows):
        position = order_buf[r]
        inside = position % half_length
        here = jnp.where(
            first,
            position // half_length,
            jnp.where(second, inside // GRID_W, inside % GRID_W),
        )
        coordinate = jnp.where(row == r, here, coordinate)
    within = jnp.where(first, pair_id, jnp.where(second, pair_id - 8, pair_id - 36))
    step = jnp.where(first, 2.0 / 16.0, 2.0 / 56.0) * (-math.log(10000.0))
    angle = coordinate.astype(jnp.float32) * jnp.exp(within.astype(jnp.float32) * step)
    cosine = jnp.cos(angle)
    sine = jnp.sin(angle)
    even = lane % 2 == 0
    sine = jnp.where(even, -sine, sine)

    def turned(values, gain):
        normed = values * rsqrt_mean(values) * gain
        swapped = jnp.where(
            even, pltpu.roll(normed, size - 1, 1), pltpu.roll(normed, 1, 1)
        )
        return normed * cosine + swapped * sine

    for i in (1, 2, 3):
        loads[i].wait()
    for h in range(heads):
        wide = slice(h * size, (h + 1) * size)
        cols = slice(h % per * size, (h % per + 1) * size)
        key = turned(ik_buf[:, wide].astype(jnp.float32), gain_buf[0])
        both = jnp.concatenate([key, iv_buf[:, wide].astype(jnp.float32)], axis=0)
        kv_own[h // per, :, cols] = both.astype(jnp.bfloat16)
    for i in (4, 5):
        loads[i].wait()
    for h in range(heads):
        wide = slice(h * size, (h + 1) * size)
        cols = slice(h % per * size, (h % per + 1) * size)
        query = turned(iq_buf[:, wide].astype(jnp.float32), gain_buf[1])
        q_own[h // per, :, cols] = query.astype(jnp.bfloat16)
    kv_all[me] = kv_own[seat]
    q_team[seat] = q_own[seat]

    pl.semaphore_wait(barrier, devices - 1)

    def remote(src, dst, send, recv, peer):
        return pltpu.make_async_remote_copy(
            src_ref=src,
            dst_ref=dst,
            send_sem=send,
            recv_sem=recv,
            device_id=(req, peer),
            device_id_type=MESH,
        )

    def kv_copy(peer, origin):
        return remote(
            kv_own.at[peer % TEAM],
            kv_all.at[origin],
            kv_send.at[peer],
            kv_recv.at[origin],
            peer,
        )

    def q_copy(peer, mate, origin):
        return remote(
            q_own.at[mate], q_team.at[origin], q_send.at[mate], q_recv.at[origin], peer
        )

    def back_copy(peer, mate, origin):
        return remote(
            back_own.at[mate],
            back_all.at[origin],
            back_send.at[mate],
            back_recv.at[origin],
            peer,
        )

    for t in range(devices // TEAM):
        for k in (3, 2, 1, 0):
            peer = t * TEAM + (seat ^ k)

            @pl.when(peer != me)
            def _():
                kv_copy(peer, me).start()

    for peer, mate in mates:
        q_copy(peer, mate, seat).start()

    for i in range(6, 12):
        loads[i].wait()

    column = lax.broadcasted_iota(jnp.int32, (1, text_rows), 1)
    bias = jnp.where(column < length_buf[0], 0.0, LOW)

    def scores_of(query, key):
        return (
            lax.dot_general(
                query, key, (((1,), (1,)), ((), ())), preferred_element_type=jnp.float32
            )
            * scale
        )

    def text_part(h, rows, query):
        cols = slice(h * size, (h + 1) * size)
        count = query.shape[0]
        scores = scores_of(query, tk_buf[:, cols]) + bias
        top = jnp.max(scores, axis=-1, keepdims=True)
        expo = jnp.exp2(scores - top)
        total = jnp.sum(expo, axis=-1, keepdims=True)
        m_buf[h, rows] = jnp.broadcast_to(top, (count, size))
        l_buf[h, rows] = jnp.broadcast_to(total, (count, size))
        o_buf[h, rows] = jnp.dot(
            expo.astype(jnp.bfloat16),
            tv_buf[:, cols],
            preferred_element_type=jnp.float32,
        )

    for h in range(per):
        cols = slice(h * size, (h + 1) * size)
        key = tk_buf[:, cols].astype(jnp.float32)
        tk_buf[:, cols] = (key * rsqrt_mean(key) * gain_buf[2]).astype(jnp.bfloat16)
        query = tq_buf[:, cols].astype(jnp.float32)
        query = (query * rsqrt_mean(query) * gain_buf[3]).astype(jnp.bfloat16)
        qs[h, :team_text] = query
        text_part(h, slice(0, team_text), query)

    for peer, mate in mates:
        q_copy(me, mate, mate).wait_recv()
    for h in range(per):
        cols = slice(h * size, (h + 1) * size)
        query = q_team[:, :, cols].astype(jnp.float32)
        query = query.reshape(TEAM * own_rows, size).astype(jnp.bfloat16)
        qs[h, team_text:] = query
        text_part(h, slice(team_text, team_rows), query)

    for d in range(1, devices):
        kv_copy(me, (me + d) % devices).wait_recv()

    def gathered(start, h):
        cols = slice(h * size, (h + 1) * size)
        whole = kv_all[:, start : start + own_rows, cols].astype(jnp.float32)
        return whole.reshape(devices * own_rows, size).astype(jnp.bfloat16)

    every = range(per)
    scores = [scores_of(qs[h], gathered(0, h)) for h in every]
    olds = [m_buf[h] for h in every]
    tops = [
        jnp.maximum(olds[h][:, :1], jnp.max(scores[h], axis=-1, keepdims=True))
        for h in every
    ]
    expos = [jnp.exp2(scores[h] - tops[h]) for h in every]
    added = [
        jnp.dot(
            expos[h].astype(jnp.bfloat16),
            gathered(own_rows, h),
            preferred_element_type=jnp.float32,
        )
        for h in every
    ]
    sums = [jnp.sum(expos[h], axis=-1, keepdims=True) for h in every]
    for h in every:
        cols = slice(h * size, (h + 1) * size)
        back = jnp.exp2(olds[h] - tops[h])
        out = (o_buf[h] * back + added[h]) / (l_buf[h] * back + sums[h])
        for s in range(TEAM):
            part = jnp.concatenate(
                [
                    out[s * share : (s + 1) * share],
                    out[team_text + s * own_rows : team_text + (s + 1) * own_rows],
                ],
                axis=0,
            )
            back_own[s, :, cols] = part.astype(jnp.bfloat16)
    for peer, mate in mates:
        back_copy(peer, mate, seat).start()
    back_all[seat] = back_own[seat]
    for peer, mate in mates:
        back_copy(me, mate, mate).wait_recv()
    out_ref[...] = back_all[...]

    for d in range(1, devices):
        kv_copy((me + d) % devices, me).wait_send()
    for peer, mate in mates:
        q_copy(peer, mate, seat).wait_send()
        back_copy(peer, mate, seat).wait_send()


def spread(parts_ref, io_ref, to_ref):
    share = to_ref.shape[0]
    span = parts_ref.shape[-1]
    for s in range(TEAM):
        cols = slice(s * span, (s + 1) * span)
        to_ref[:, cols] = parts_ref[s, :share]
        io_ref[:, cols] = parts_ref[s, share:]


def local(iq, ik, iv, tq, tk, tv, iqg, ikg, tqg, tkg, order, length):
    devices = lax.axis_size("seq")
    own_rows, width = iq.shape
    size = iqg.shape[0]
    span = width // TEAM
    per = span // size
    text_rows = tq.shape[0]
    share = text_rows // devices
    team_text = share * TEAM
    team_rows = team_text + TEAM * own_rows
    vmem = pl.BlockSpec(memory_space=pltpu.VMEM)
    hbm = pl.BlockSpec(memory_space=pl.ANY)
    gains = [g.reshape(1, size) for g in (iqg, ikg, tqg, tkg)]
    bf16, f32 = jnp.bfloat16, jnp.float32
    parts = pl.pallas_call(
        functools.partial(kernel, devices),
        out_shape=pltpu.VMEM((TEAM, share + own_rows, span), bf16),
        in_specs=[hbm] * 12,
        out_specs=vmem,
        scratch_shapes=[
            pltpu.VMEM((own_rows, width), bf16),
            pltpu.VMEM((own_rows, width), bf16),
            pltpu.VMEM((own_rows, width), bf16),
            pltpu.VMEM((team_text, span), bf16),
            pltpu.VMEM((text_rows, span), bf16),
            pltpu.VMEM((text_rows, span), bf16),
            pltpu.VMEM((4, 1, size), f32),
            pltpu.SMEM((own_rows,), jnp.int32),
            pltpu.SMEM((1,), jnp.int32),
            pltpu.VMEM((TEAM, 2 * own_rows, span), bf16),
            pltpu.VMEM((TEAM, own_rows, span), bf16),
            pltpu.VMEM((devices, 2 * own_rows, span), bf16),
            pltpu.VMEM((TEAM, own_rows, span), bf16),
            pltpu.VMEM((per, team_rows, size), bf16),
            pltpu.VMEM((per, team_rows, size), f32),
            pltpu.VMEM((per, team_rows, size), f32),
            pltpu.VMEM((per, team_rows, size), f32),
            pltpu.VMEM((TEAM, share + own_rows, span), bf16),
            pltpu.VMEM((TEAM, share + own_rows, span), bf16),
            pltpu.SemaphoreType.DMA((12,)),
            pltpu.SemaphoreType.DMA((devices,)),
            pltpu.SemaphoreType.DMA((devices,)),
            pltpu.SemaphoreType.DMA((TEAM,)),
            pltpu.SemaphoreType.DMA((TEAM,)),
            pltpu.SemaphoreType.DMA((TEAM,)),
            pltpu.SemaphoreType.DMA((TEAM,)),
        ],
        compiler_params=pltpu.CompilerParams(
            collective_id=0, has_side_effects=True, vmem_limit_bytes=32 * 1024 * 1024
        ),
    )(iq, ik, iv, tq, tk, tv, *gains, order, length)
    parts = pltpu.with_memory_space_constraint(parts, pltpu.VMEM)
    return pl.pallas_call(
        spread,
        out_shape=(
            jax.ShapeDtypeStruct((own_rows, width), bf16),
            jax.ShapeDtypeStruct((share, width), bf16),
        ),
        in_specs=[vmem],
        out_specs=(vmem, vmem),
    )(parts)


def solution(mesh):
    rows = P(("req", "seq"), None)
    text = P("req", None)
    return jax.shard_map(
        local,
        mesh=mesh,
        in_specs=(rows, rows, rows, text, text, text)
        + (P(), P(), P(), P(), P(("req", "seq")), P("req")),
        out_specs=(rows, rows),
        check_vma=False,
    )
```

```python
import functools
import math

import jax
import jax.numpy as jnp
from jax import lax
from jax.experimental import pallas as pl
from jax.experimental.pallas import tpu as pltpu
from jax.sharding import PartitionSpec as P

GRID_W = 64
EPS = 1e-06
LOW = -1e30
TEAM = 4
MESH = pl.DeviceIdType.MESH


def rsqrt_mean(values):
    return lax.rsqrt(jnp.mean(values * values, axis=-1, keepdims=True) + EPS)


def kernel(
    devices,
    iq_ref,
    ik_ref,
    iv_ref,
    tq_ref,
    tk_ref,
    tv_ref,
    iqg_ref,
    ikg_ref,
    tqg_ref,
    tkg_ref,
    order_ref,
    length_ref,
    out_ref,
    iq_buf,
    ik_buf,
    iv_buf,
    tq_buf,
    tk_buf,
    tv_buf,
    gain_buf,
    order_buf,
    length_buf,
    kv_own,
    q_own,
    kv_all,
    q_team,
    qs,
    m_buf,
    l_buf,
    o_buf,
    back_own,
    back_all,
    local_sem,
    kv_send,
    kv_recv,
    q_send,
    q_recv,
    back_send,
    back_recv,
):
    me = lax.axis_index("seq")
    req = lax.axis_index("req")
    seat = me % TEAM
    team = me // TEAM
    mates = [(team * TEAM + (seat ^ k), seat ^ k) for k in (3, 2, 1)]

    barrier = pltpu.get_barrier_semaphore()
    for d in range(1, devices):
        pl.semaphore_signal(
            barrier, inc=1, device_id=(req, (me + d) % devices), device_id_type=MESH
        )

    own_rows, width = iq_buf.shape
    size = gain_buf.shape[-1]
    heads = width // size
    text_rows, span = tk_buf.shape
    per = span // size
    team_text = tq_buf.shape[0]
    share = team_text // TEAM
    team_rows = team_text + TEAM * own_rows
    scale = math.log2(math.e) / math.sqrt(size)

    lanes = pl.ds(pl.multiple_of(seat * span, span), span)
    text = pl.ds(pl.multiple_of(team * team_text, team_text), team_text)
    loads = []
    for src, dst in (
        (order_ref, order_buf),
        (ik_ref, ik_buf),
        (ikg_ref, gain_buf.at[0]),
        (iv_ref, iv_buf),
        (iq_ref, iq_buf),
        (iqg_ref, gain_buf.at[1]),
        (tk_ref.at[:, lanes], tk_buf),
        (tkg_ref, gain_buf.at[2]),
        (tq_ref.at[text, lanes], tq_buf),
        (tqg_ref, gain_buf.at[3]),
        (length_ref, length_buf),
        (tv_ref.at[:, lanes], tv_buf),
    ):
        copy = pltpu.make_async_copy(src, dst, local_sem.at[len(loads)])
        copy.start()
        loads.append(copy)

    loads[0].wait()
    half_length = own_rows * devices // 2
    lane = lax.broadcasted_iota(jnp.int32, (own_rows, size), 1)
    row = lax.broadcasted_iota(jnp.int32, (own_rows, size), 0)
    pair_id = lane // 2
    first = pair_id < 8
    second = pair_id < 36
    coordinate = jnp.zeros((own_rows, size), jnp.int32)
    for r in range(own_rows):
        position = order_buf[r]
        inside = position % half_length
        here = jnp.where(
            first,
            position // half_length,
            jnp.where(second, inside // GRID_W, inside % GRID_W),
        )
        coordinate = jnp.where(row == r, here, coordinate)
    within = jnp.where(first, pair_id, jnp.where(second, pair_id - 8, pair_id - 36))
    step = jnp.where(first, 2.0 / 16.0, 2.0 / 56.0) * (-math.log(10000.0))
    angle = coordinate.astype(jnp.float32) * jnp.exp(within.astype(jnp.float32) * step)
    cosine = jnp.cos(angle)
    sine = jnp.sin(angle)
    even = lane % 2 == 0
    sine = jnp.where(even, -sine, sine)

    def turned(values, gain):
        normed = values * rsqrt_mean(values) * gain
        swapped = jnp.where(
            even, pltpu.roll(normed, size - 1, 1), pltpu.roll(normed, 1, 1)
        )
        return normed * cosine + swapped * sine

    for i in (1, 2, 3):
        loads[i].wait()
    for h in range(heads):
        wide = slice(h * size, (h + 1) * size)
        cols = slice(h % per * size, (h % per + 1) * size)
        key = turned(ik_buf[:, wide].astype(jnp.float32), gain_buf[0])
        both = jnp.concatenate([key, iv_buf[:, wide].astype(jnp.float32)], axis=0)
        kv_own[h // per, :, cols] = both.astype(jnp.bfloat16)
    for i in (4, 5):
        loads[i].wait()
    for h in range(heads):
        wide = slice(h * size, (h + 1) * size)
        cols = slice(h % per * size, (h % per + 1) * size)
        query = turned(iq_buf[:, wide].astype(jnp.float32), gain_buf[1])
        q_own[h // per, :, cols] = query.astype(jnp.bfloat16)
    kv_all[me] = kv_own[seat]
    q_team[seat] = q_own[seat]

    pl.semaphore_wait(barrier, devices - 1)

    def remote(src, dst, send, recv, peer):
        return pltpu.make_async_remote_copy(
            src_ref=src,
            dst_ref=dst,
            send_sem=send,
            recv_sem=recv,
            device_id=(req, peer),
            device_id_type=MESH,
        )

    def kv_copy(peer, origin):
        return remote(
            kv_own.at[peer % TEAM],
            kv_all.at[origin],
            kv_send.at[peer],
            kv_recv.at[origin],
            peer,
        )

    def q_copy(peer, mate, origin):
        return remote(
            q_own.at[mate], q_team.at[origin], q_send.at[mate], q_recv.at[origin], peer
        )

    def back_copy(peer, mate, origin):
        return remote(
            back_own.at[mate],
            back_all.at[origin],
            back_send.at[mate],
            back_recv.at[origin],
            peer,
        )

    for t in range(devices // TEAM):
        for k in (3, 2, 1, 0):
            peer = t * TEAM + (seat ^ k)

            @pl.when(peer != me)
            def _():
                kv_copy(peer, me).start()

    for peer, mate in mates:
        q_copy(peer, mate, seat).start()

    for i in range(6, 12):
        loads[i].wait()

    column = lax.broadcasted_iota(jnp.int32, (1, text_rows), 1)
    bias = jnp.where(column < length_buf[0], 0.0, LOW)

    def scores_of(query, key):
        return (
            lax.dot_general(
                query, key, (((1,), (1,)), ((), ())), preferred_element_type=jnp.float32
            )
            * scale
        )

    def text_part(h, rows, query):
        cols = slice(h * size, (h + 1) * size)
        count = query.shape[0]
        scores = scores_of(query, tk_buf[:, cols]) + bias
        top = jnp.max(scores, axis=-1, keepdims=True)
        expo = jnp.exp2(scores - top)
        total = jnp.sum(expo, axis=-1, keepdims=True)
        m_buf[h, rows] = jnp.broadcast_to(top, (count, size))
        l_buf[h, rows] = jnp.broadcast_to(total, (count, size))
        o_buf[h, rows] = jnp.dot(
            expo.astype(jnp.bfloat16),
            tv_buf[:, cols],
            preferred_element_type=jnp.float32,
        )

    for h in range(per):
        cols = slice(h * size, (h + 1) * size)
        key = tk_buf[:, cols].astype(jnp.float32)
        tk_buf[:, cols] = (key * rsqrt_mean(key) * gain_buf[2]).astype(jnp.bfloat16)
        query = tq_buf[:, cols].astype(jnp.float32)
        query = (query * rsqrt_mean(query) * gain_buf[3]).astype(jnp.bfloat16)
        qs[h, :team_text] = query
        text_part(h, slice(0, team_text), query)

    for peer, mate in mates:
        q_copy(me, mate, mate).wait_recv()
    for h in range(per):
        cols = slice(h * size, (h + 1) * size)
        query = q_team[:, :, cols].astype(jnp.float32)
        query = query.reshape(TEAM * own_rows, size).astype(jnp.bfloat16)
        qs[h, team_text:] = query
        text_part(h, slice(team_text, team_rows), query)

    for d in range(1, devices):
        kv_copy(me, (me + d) % devices).wait_recv()

    def gathered(start, h):
        cols = slice(h * size, (h + 1) * size)
        whole = kv_all[:, start : start + own_rows, cols].astype(jnp.float32)
        return whole.reshape(devices * own_rows, size).astype(jnp.bfloat16)

    every = range(per)
    scores = [scores_of(qs[h], gathered(0, h)) for h in every]
    olds = [m_buf[h] for h in every]
    tops = [
        jnp.maximum(olds[h][:, :1], jnp.max(scores[h], axis=-1, keepdims=True))
        for h in every
    ]
    expos = [jnp.exp2(scores[h] - tops[h]) for h in every]
    added = [
        jnp.dot(
            expos[h].astype(jnp.bfloat16),
            gathered(own_rows, h),
            preferred_element_type=jnp.float32,
        )
        for h in every
    ]
    sums = [jnp.sum(expos[h], axis=-1, keepdims=True) for h in every]
    for h in every:
        cols = slice(h * size, (h + 1) * size)
        back = jnp.exp2(olds[h] - tops[h])
        out = (o_buf[h] * back + added[h]) / (l_buf[h] * back + sums[h])
        for s in range(TEAM):
            part = jnp.concatenate(
                [
                    out[s * share : (s + 1) * share],
                    out[team_text + s * own_rows : team_text + (s + 1) * own_rows],
                ],
                axis=0,
            )
            back_own[s, :, cols] = part.astype(jnp.bfloat16)
    for peer, mate in mates:
        back_copy(peer, mate, seat).start()
    back_all[seat] = back_own[seat]
    for peer, mate in mates:
        back_copy(me, mate, mate).wait_recv()
    out_ref[...] = back_all[...]

    for d in range(1, devices):
        kv_copy((me + d) % devices, me).wait_send()
    for peer, mate in mates:
        q_copy(peer, mate, seat).wait_send()
        back_copy(peer, mate, seat).wait_send()


def spread(parts_ref, io_ref, to_ref):
    share = to_ref.shape[0]
    span = parts_ref.shape[-1]
    for s in range(TEAM):
        cols = slice(s * span, (s + 1) * span)
        to_ref[:, cols] = parts_ref[s, :share]
        io_ref[:, cols] = parts_ref[s, share:]


def local(iq, ik, iv, tq, tk, tv, iqg, ikg, tqg, tkg, order, length):
    devices = lax.axis_size("seq")
    own_rows, width = iq.shape
    size = iqg.shape[0]
    span = width // TEAM
    per = span // size
    text_rows = tq.shape[0]
    share = text_rows // devices
    team_text = share * TEAM
    team_rows = team_text + TEAM * own_rows
    vmem = pl.BlockSpec(memory_space=pltpu.VMEM)
    hbm = pl.BlockSpec(memory_space=pl.ANY)
    gains = [g.reshape(1, size) for g in (iqg, ikg, tqg, tkg)]
    bf16, f32 = jnp.bfloat16, jnp.float32
    parts = pl.pallas_call(
        functools.partial(kernel, devices),
        out_shape=pltpu.VMEM((TEAM, share + own_rows, span), bf16),
        in_specs=[hbm] * 12,
        out_specs=vmem,
        scratch_shapes=[
            pltpu.VMEM((own_rows, width), bf16),
            pltpu.VMEM((own_rows, width), bf16),
            pltpu.VMEM((own_rows, width), bf16),
            pltpu.VMEM((team_text, span), bf16),
            pltpu.VMEM((text_rows, span), bf16),
            pltpu.VMEM((text_rows, span), bf16),
            pltpu.VMEM((4, 1, size), f32),
            pltpu.SMEM((own_rows,), jnp.int32),
            pltpu.SMEM((1,), jnp.int32),
            pltpu.VMEM((TEAM, 2 * own_rows, span), bf16),
            pltpu.VMEM((TEAM, own_rows, span), bf16),
            pltpu.VMEM((devices, 2 * own_rows, span), bf16),
            pltpu.VMEM((TEAM, own_rows, span), bf16),
            pltpu.VMEM((per, team_rows, size), bf16),
            pltpu.VMEM((per, team_rows, size), f32),
            pltpu.VMEM((per, team_rows, size), f32),
            pltpu.VMEM((per, team_rows, size), f32),
            pltpu.VMEM((TEAM, share + own_rows, span), bf16),
            pltpu.VMEM((TEAM, share + own_rows, span), bf16),
            pltpu.SemaphoreType.DMA((12,)),
            pltpu.SemaphoreType.DMA((devices,)),
            pltpu.SemaphoreType.DMA((devices,)),
            pltpu.SemaphoreType.DMA((TEAM,)),
            pltpu.SemaphoreType.DMA((TEAM,)),
            pltpu.SemaphoreType.DMA((TEAM,)),
            pltpu.SemaphoreType.DMA((TEAM,)),
        ],
        compiler_params=pltpu.CompilerParams(
            collective_id=0, has_side_effects=True, vmem_limit_bytes=62 * 1024 * 1024
        ),
    )(iq, ik, iv, tq, tk, tv, *gains, order, length)
    parts = pltpu.with_memory_space_constraint(parts, pltpu.VMEM)
    return pl.pallas_call(
        spread,
        out_shape=(
            jax.ShapeDtypeStruct((own_rows, width), bf16),
            jax.ShapeDtypeStruct((share, width), bf16),
        ),
        in_specs=[vmem],
        out_specs=(vmem, vmem),
    )(parts)


def solution(mesh):
    rows = P(("req", "seq"), None)
    text = P("req", None)
    return jax.shard_map(
        local,
        mesh=mesh,
        in_specs=(rows, rows, rows, text, text, text)
        + (P(), P(), P(), P(), P(("req", "seq")), P("req")),
        out_specs=(rows, rows),
        check_vma=False,
    )
```

```python
import functools
import math

import jax
import jax.numpy as jnp
from jax import lax
from jax.experimental import pallas as pl
from jax.experimental.pallas import tpu as pltpu
from jax.sharding import PartitionSpec as P

GRID_W = 64
EPS = 1e-06
LOW = -1e30
TEAM = 4
MESH = pl.DeviceIdType.MESH


def rsqrt_mean(values):
    return lax.rsqrt(jnp.mean(values * values, axis=-1, keepdims=True) + EPS)


def kernel(
    devices,
    iq_ref,
    ik_ref,
    iv_ref,
    tq_ref,
    tk_ref,
    tv_ref,
    iqg_ref,
    ikg_ref,
    tqg_ref,
    tkg_ref,
    order_ref,
    length_ref,
    out_ref,
    iq_buf,
    ik_buf,
    iv_buf,
    tq_buf,
    tk_buf,
    tv_buf,
    gain_buf,
    order_buf,
    length_buf,
    kv_own,
    q_own,
    kv_all,
    q_team,
    qs,
    m_buf,
    l_buf,
    o_buf,
    back_own,
    back_all,
    local_sem,
    kv_send,
    kv_recv,
    ready_sem,
    q_send,
    q_recv,
    back_send,
    back_recv,
):
    me = lax.axis_index("seq")
    req = lax.axis_index("req")
    seat = me % TEAM
    team = me // TEAM
    mates = [(team * TEAM + (seat ^ k), seat ^ k) for k in (3, 2, 1)]

    barrier = pltpu.get_barrier_semaphore()
    teams = devices // TEAM
    last = teams - 1
    gate = teams - 2
    for t in reversed(range(teams)):
        direct = (team < last) | (t >= gate)
        for k in (3, 2, 1, 0):
            peer = t * TEAM + (seat ^ k)

            @pl.when((peer != me) & direct)
            def _():
                pl.semaphore_signal(
                    barrier, inc=1, device_id=(req, peer), device_id_type=MESH
                )

    own_rows, width = iq_buf.shape
    size = gain_buf.shape[-1]
    heads = width // size
    text_rows, span = tk_buf.shape
    per = span // size
    team_text = tq_buf.shape[0]
    share = team_text // TEAM
    team_rows = team_text + TEAM * own_rows
    scale = math.log2(math.e) / math.sqrt(size)

    lanes = pl.ds(pl.multiple_of(seat * span, span), span)
    text = pl.ds(pl.multiple_of(team * team_text, team_text), team_text)
    loads = []
    for src, dst in (
        (order_ref, order_buf),
        (ik_ref, ik_buf),
        (ikg_ref, gain_buf.at[0]),
        (iv_ref, iv_buf),
        (iq_ref, iq_buf),
        (iqg_ref, gain_buf.at[1]),
        (tk_ref.at[:, lanes], tk_buf),
        (tkg_ref, gain_buf.at[2]),
        (tq_ref.at[text, lanes], tq_buf),
        (tqg_ref, gain_buf.at[3]),
        (length_ref, length_buf),
        (tv_ref.at[:, lanes], tv_buf),
    ):
        copy = pltpu.make_async_copy(src, dst, local_sem.at[len(loads)])
        copy.start()
        loads.append(copy)

    loads[0].wait()
    half_length = own_rows * devices // 2
    lane = lax.broadcasted_iota(jnp.int32, (own_rows, size), 1)
    row = lax.broadcasted_iota(jnp.int32, (own_rows, size), 0)
    pair_id = lane // 2
    first = pair_id < 8
    second = pair_id < 36
    coordinate = jnp.zeros((own_rows, size), jnp.int32)
    for r in range(own_rows):
        position = order_buf[r]
        inside = position % half_length
        here = jnp.where(
            first,
            position // half_length,
            jnp.where(second, inside // GRID_W, inside % GRID_W),
        )
        coordinate = jnp.where(row == r, here, coordinate)
    within = jnp.where(first, pair_id, jnp.where(second, pair_id - 8, pair_id - 36))
    step = jnp.where(first, 2.0 / 16.0, 2.0 / 56.0) * (-math.log(10000.0))
    angle = coordinate.astype(jnp.float32) * jnp.exp(within.astype(jnp.float32) * step)
    cosine = jnp.cos(angle)
    sine = jnp.sin(angle)
    even = lane % 2 == 0
    sine = jnp.where(even, -sine, sine)

    def turned(values, gain):
        normed = values * rsqrt_mean(values) * gain
        swapped = jnp.where(
            even, pltpu.roll(normed, size - 1, 1), pltpu.roll(normed, 1, 1)
        )
        return normed * cosine + swapped * sine

    for i in (1, 2, 3):
        loads[i].wait()
    for h in range(heads):
        wide = slice(h * size, (h + 1) * size)
        cols = slice(h % per * size, (h % per + 1) * size)
        key = turned(ik_buf[:, wide].astype(jnp.float32), gain_buf[0])
        both = jnp.concatenate([key, iv_buf[:, wide].astype(jnp.float32)], axis=0)
        kv_own[h // per, :, cols] = both.astype(jnp.bfloat16)

    pl.semaphore_wait(
        barrier, jnp.where(team < gate, devices - 1 - TEAM, devices - 1)
    )

    def remote(src, dst, send, recv, peer):
        return pltpu.make_async_remote_copy(
            src_ref=src,
            dst_ref=dst,
            send_sem=send,
            recv_sem=recv,
            device_id=(req, peer),
            device_id_type=MESH,
        )

    def kv_copy(peer, origin):
        return remote(
            kv_own.at[peer % TEAM],
            kv_all.at[origin],
            kv_send.at[peer],
            kv_recv.at[origin],
            peer,
        )

    def q_copy(peer, mate, origin):
        return remote(
            q_own.at[mate], q_team.at[origin], q_send.at[mate], q_recv.at[origin], peer
        )

    def back_copy(peer, mate, origin):
        return remote(
            back_own.at[mate],
            back_all.at[origin],
            back_send.at[mate],
            back_recv.at[origin],
            peer,
        )

    @pl.when(team == gate)
    def _():
        for t in range(gate):
            pl.semaphore_signal(
                ready_sem, inc=1, device_id=(req, t * TEAM + seat), device_id_type=MESH
            )

    def feed(t, allowed):
        for k in (3, 2, 1, 0):
            peer = t * TEAM + (seat ^ k)

            @pl.when((peer != me) & allowed)
            def _():
                kv_copy(peer, me).start()

    for t in range(last):
        feed(t, True)
    feed(last, team >= gate)

    for i in (4, 5):
        loads[i].wait()
    for h in range(heads):
        wide = slice(h * size, (h + 1) * size)
        cols = slice(h % per * size, (h % per + 1) * size)
        query = turned(iq_buf[:, wide].astype(jnp.float32), gain_buf[1])
        q_own[h // per, :, cols] = query.astype(jnp.bfloat16)
    for peer, mate in mates:
        q_copy(peer, mate, seat).start()
    kv_all[me] = kv_own[seat]
    q_team[seat] = q_own[seat]

    @pl.when(team < gate)
    def _():
        pl.semaphore_wait(ready_sem, 1)

    feed(last, team < gate)

    for i in range(6, 12):
        loads[i].wait()

    column = lax.broadcasted_iota(jnp.int32, (1, text_rows), 1)
    bias = jnp.where(column < length_buf[0], 0.0, LOW)

    def scores_of(query, key):
        return (
            lax.dot_general(
                query, key, (((1,), (1,)), ((), ())), preferred_element_type=jnp.float32
            )
            * scale
        )

    def text_part(h, rows, query):
        cols = slice(h * size, (h + 1) * size)
        count = query.shape[0]
        scores = scores_of(query, tk_buf[:, cols]) + bias
        top = jnp.max(scores, axis=-1, keepdims=True)
        expo = jnp.exp2(scores - top)
        total = jnp.sum(expo, axis=-1, keepdims=True)
        m_buf[h, rows] = jnp.broadcast_to(top, (count, size))
        l_buf[h, rows] = jnp.broadcast_to(total, (count, size))
        o_buf[h, rows] = jnp.dot(
            expo.astype(jnp.bfloat16),
            tv_buf[:, cols],
            preferred_element_type=jnp.float32,
        )

    for h in range(per):
        cols = slice(h * size, (h + 1) * size)
        key = tk_buf[:, cols].astype(jnp.float32)
        tk_buf[:, cols] = (key * rsqrt_mean(key) * gain_buf[2]).astype(jnp.bfloat16)
        query = tq_buf[:, cols].astype(jnp.float32)
        query = (query * rsqrt_mean(query) * gain_buf[3]).astype(jnp.bfloat16)
        qs[h, :team_text] = query
        text_part(h, slice(0, team_text), query)

    for peer, mate in mates:
        q_copy(me, mate, mate).wait_recv()
    for h in range(per):
        cols = slice(h * size, (h + 1) * size)
        query = q_team[:, :, cols].astype(jnp.float32)
        query = query.reshape(TEAM * own_rows, size).astype(jnp.bfloat16)
        qs[h, team_text:] = query
        text_part(h, slice(team_text, team_rows), query)

    for t in range(teams):
        for k in (0, 1, 2, 3):
            origin = t * TEAM + (seat ^ k)

            @pl.when(origin != me)
            def _():
                kv_copy(me, origin).wait_recv()

    def gathered(start, h):
        cols = slice(h * size, (h + 1) * size)
        whole = kv_all[:, start : start + own_rows, cols].astype(jnp.float32)
        return whole.reshape(devices * own_rows, size).astype(jnp.bfloat16)

    every = range(per)
    scores = [scores_of(qs[h], gathered(0, h)) for h in every]
    olds = [m_buf[h] for h in every]
    tops = [
        jnp.maximum(olds[h][:, :1], jnp.max(scores[h], axis=-1, keepdims=True))
        for h in every
    ]
    expos = [jnp.exp2(scores[h] - tops[h]) for h in every]
    added = [
        jnp.dot(
            expos[h].astype(jnp.bfloat16),
            gathered(own_rows, h),
            preferred_element_type=jnp.float32,
        )
        for h in every
    ]
    sums = [jnp.sum(expos[h], axis=-1, keepdims=True) for h in every]
    for h in every:
        cols = slice(h * size, (h + 1) * size)
        back = jnp.exp2(olds[h] - tops[h])
        out = (o_buf[h] * back + added[h]) / (l_buf[h] * back + sums[h])
        for s in range(TEAM):
            part = jnp.concatenate(
                [
                    out[s * share : (s + 1) * share],
                    out[team_text + s * own_rows : team_text + (s + 1) * own_rows],
                ],
                axis=0,
            )
            back_own[s, :, cols] = part.astype(jnp.bfloat16)
    for mate in range(TEAM):

        @pl.when(mate != seat)
        def _():
            back_copy(team * TEAM + mate, mate, seat).start()

    back_all[seat] = back_own[seat]
    for d in range(1, devices):
        kv_copy((me + d) % devices, me).wait_send()
    for peer, mate in mates:
        q_copy(peer, mate, seat).wait_send()
    for peer, mate in mates:
        back_copy(me, mate, mate).wait_recv()
    out_ref[...] = back_all[...]

    for peer, mate in mates:
        back_copy(peer, mate, seat).wait_send()


def spread(parts_ref, io_ref, to_ref):
    share = to_ref.shape[0]
    span = parts_ref.shape[-1]
    for s in range(TEAM):
        cols = slice(s * span, (s + 1) * span)
        to_ref[:, cols] = parts_ref[s, :share]
        io_ref[:, cols] = parts_ref[s, share:]


def local(iq, ik, iv, tq, tk, tv, iqg, ikg, tqg, tkg, order, length):
    devices = lax.axis_size("seq")
    own_rows, width = iq.shape
    size = iqg.shape[0]
    span = width // TEAM
    per = span // size
    text_rows = tq.shape[0]
    share = text_rows // devices
    team_text = share * TEAM
    team_rows = team_text + TEAM * own_rows
    vmem = pl.BlockSpec(memory_space=pltpu.VMEM)
    hbm = pl.BlockSpec(memory_space=pl.ANY)
    gains = [g.reshape(1, size) for g in (iqg, ikg, tqg, tkg)]
    bf16, f32 = jnp.bfloat16, jnp.float32
    parts = pl.pallas_call(
        functools.partial(kernel, devices),
        out_shape=pltpu.VMEM((TEAM, share + own_rows, span), bf16),
        in_specs=[hbm] * 12,
        out_specs=vmem,
        scratch_shapes=[
            pltpu.VMEM((own_rows, width), bf16),
            pltpu.VMEM((own_rows, width), bf16),
            pltpu.VMEM((own_rows, width), bf16),
            pltpu.VMEM((team_text, span), bf16),
            pltpu.VMEM((text_rows, span), bf16),
            pltpu.VMEM((text_rows, span), bf16),
            pltpu.VMEM((4, 1, size), f32),
            pltpu.SMEM((own_rows,), jnp.int32),
            pltpu.SMEM((1,), jnp.int32),
            pltpu.VMEM((TEAM, 2 * own_rows, span), bf16),
            pltpu.VMEM((TEAM, own_rows, span), bf16),
            pltpu.VMEM((devices, 2 * own_rows, span), bf16),
            pltpu.VMEM((TEAM, own_rows, span), bf16),
            pltpu.VMEM((per, team_rows, size), bf16),
            pltpu.VMEM((per, team_rows, size), f32),
            pltpu.VMEM((per, team_rows, size), f32),
            pltpu.VMEM((per, team_rows, size), f32),
            pltpu.VMEM((TEAM, share + own_rows, span), bf16),
            pltpu.VMEM((TEAM, share + own_rows, span), bf16),
            pltpu.SemaphoreType.DMA((12,)),
            pltpu.SemaphoreType.DMA((devices,)),
            pltpu.SemaphoreType.DMA((devices,)),
            pltpu.SemaphoreType.REGULAR,
            pltpu.SemaphoreType.DMA((TEAM,)),
            pltpu.SemaphoreType.DMA((TEAM,)),
            pltpu.SemaphoreType.DMA((TEAM,)),
            pltpu.SemaphoreType.DMA((TEAM,)),
        ],
        compiler_params=pltpu.CompilerParams(
            collective_id=0, has_side_effects=True, vmem_limit_bytes=62 * 1024 * 1024
        ),
    )(iq, ik, iv, tq, tk, tv, *gains, order, length)
    parts = pltpu.with_memory_space_constraint(parts, pltpu.VMEM)
    return pl.pallas_call(
        spread,
        out_shape=(
            jax.ShapeDtypeStruct((own_rows, width), bf16),
            jax.ShapeDtypeStruct((share, width), bf16),
        ),
        in_specs=[vmem],
        out_specs=(vmem, vmem),
    )(parts)


def solution(mesh):
    rows = P(("req", "seq"), None)
    text = P("req", None)
    return jax.shard_map(
        local,
        mesh=mesh,
        in_specs=(rows, rows, rows, text, text, text)
        + (P(), P(), P(), P(), P(("req", "seq")), P("req")),
        out_specs=(rows, rows),
        check_vma=False,
    )
```

```python
import functools
import math

import jax
import jax.numpy as jnp
from jax import lax
from jax.experimental import pallas as pl
from jax.experimental.pallas import tpu as pltpu
from jax.sharding import PartitionSpec as P

GRID_W = 64
EPS = 1e-06
LOW = -1e30
TEAM = 4
ORDERS = ((3, 2, 1, 0), (3, 2, 1, 0), (3, 1, 2, 0), (3, 2, 1, 0))
MESH = pl.DeviceIdType.MESH


def rsqrt_mean(values):
    return lax.rsqrt(jnp.mean(values * values, axis=-1, keepdims=True) + EPS)


def kernel(
    devices,
    iq_ref,
    ik_ref,
    iv_ref,
    tq_ref,
    tk_ref,
    tv_ref,
    iqg_ref,
    ikg_ref,
    tqg_ref,
    tkg_ref,
    order_ref,
    length_ref,
    out_ref,
    iq_buf,
    ik_buf,
    iv_buf,
    tq_buf,
    tk_buf,
    tv_buf,
    gain_buf,
    order_buf,
    length_buf,
    kv_own,
    q_own,
    kv_all,
    q_team,
    qs,
    m_buf,
    l_buf,
    o_buf,
    back_own,
    back_all,
    local_sem,
    kv_send,
    kv_recv,
    ready_sem,
    q_send,
    q_recv,
    back_send,
    back_recv,
):
    me = lax.axis_index("seq")
    req = lax.axis_index("req")
    seat = me % TEAM
    team = me // TEAM
    mates = [(team * TEAM + (seat ^ k), seat ^ k) for k in (3, 2, 1)]

    barrier = pltpu.get_barrier_semaphore()
    teams = devices // TEAM
    last = teams - 1
    for t in reversed(range(teams)):
        for k in (3, 2, 1, 0):
            peer = t * TEAM + (seat ^ k)

            @pl.when((peer != me) & (t >= team))
            def _():
                pl.semaphore_signal(
                    barrier, inc=1, device_id=(req, peer), device_id_type=MESH
                )

    own_rows, width = iq_buf.shape
    size = gain_buf.shape[-1]
    heads = width // size
    text_rows, span = tk_buf.shape
    per = span // size
    team_text = tq_buf.shape[0]
    share = team_text // TEAM
    team_rows = team_text + TEAM * own_rows
    scale = math.log2(math.e) / math.sqrt(size)

    lanes = pl.ds(pl.multiple_of(seat * span, span), span)
    text = pl.ds(pl.multiple_of(team * team_text, team_text), team_text)
    loads = []
    for src, dst in (
        (order_ref, order_buf),
        (ik_ref, ik_buf),
        (ikg_ref, gain_buf.at[0]),
        (iv_ref, iv_buf),
        (iq_ref, iq_buf),
        (iqg_ref, gain_buf.at[1]),
        (tk_ref.at[:, lanes], tk_buf),
        (tkg_ref, gain_buf.at[2]),
        (tq_ref.at[text, lanes], tq_buf),
        (tqg_ref, gain_buf.at[3]),
        (length_ref, length_buf),
        (tv_ref.at[:, lanes], tv_buf),
    ):
        copy = pltpu.make_async_copy(src, dst, local_sem.at[len(loads)])
        copy.start()
        loads.append(copy)

    loads[0].wait()
    half_length = own_rows * devices // 2
    lane = lax.broadcasted_iota(jnp.int32, (own_rows, size), 1)
    row = lax.broadcasted_iota(jnp.int32, (own_rows, size), 0)
    pair_id = lane // 2
    first = pair_id < 8
    second = pair_id < 36
    coordinate = jnp.zeros((own_rows, size), jnp.int32)
    for r in range(own_rows):
        position = order_buf[r]
        inside = position % half_length
        here = jnp.where(
            first,
            position // half_length,
            jnp.where(second, inside // GRID_W, inside % GRID_W),
        )
        coordinate = jnp.where(row == r, here, coordinate)
    within = jnp.where(first, pair_id, jnp.where(second, pair_id - 8, pair_id - 36))
    step = jnp.where(first, 2.0 / 16.0, 2.0 / 56.0) * (-math.log(10000.0))
    angle = coordinate.astype(jnp.float32) * jnp.exp(within.astype(jnp.float32) * step)
    cosine = jnp.cos(angle)
    sine = jnp.sin(angle)
    even = lane % 2 == 0
    sine = jnp.where(even, -sine, sine)

    def turned(values, gain):
        normed = values * rsqrt_mean(values) * gain
        swapped = jnp.where(
            even, pltpu.roll(normed, size - 1, 1), pltpu.roll(normed, 1, 1)
        )
        return normed * cosine + swapped * sine

    for i in (1, 2, 3):
        loads[i].wait()
    for h in range(heads):
        wide = slice(h * size, (h + 1) * size)
        cols = slice(h % per * size, (h % per + 1) * size)
        key = turned(ik_buf[:, wide].astype(jnp.float32), gain_buf[0])
        both = jnp.concatenate([key, iv_buf[:, wide].astype(jnp.float32)], axis=0)
        kv_own[h // per, :, cols] = both.astype(jnp.bfloat16)

    pl.semaphore_wait(barrier, (team + 1) * TEAM - 1)

    def remote(src, dst, send, recv, peer):
        return pltpu.make_async_remote_copy(
            src_ref=src,
            dst_ref=dst,
            send_sem=send,
            recv_sem=recv,
            device_id=(req, peer),
            device_id_type=MESH,
        )

    def kv_copy(peer, origin):
        return remote(
            kv_own.at[peer % TEAM],
            kv_all.at[origin],
            kv_send.at[peer],
            kv_recv.at[origin],
            peer,
        )

    def q_copy(peer, mate, origin):
        return remote(
            q_own.at[mate], q_team.at[origin], q_send.at[mate], q_recv.at[origin], peer
        )

    def back_copy(peer, mate, origin):
        return remote(
            back_own.at[mate],
            back_all.at[origin],
            back_send.at[mate],
            back_recv.at[origin],
            peer,
        )

    for t in range(last):

        @pl.when(t < team)
        def _():
            pl.semaphore_signal(
                ready_sem.at[team],
                inc=1,
                device_id=(req, t * TEAM + seat),
                device_id_type=MESH,
            )

    def pick(values):
        value = values[-1]
        for place in reversed(range(TEAM - 1)):
            value = jnp.where(seat == place, values[place], value)
        return value

    places = [pick(column) for column in zip(*ORDERS)]

    def feed(t, allowed):
        for place in places:
            peer = t * TEAM + place

            @pl.when((peer != me) & allowed)
            def _():
                kv_copy(peer, me).start()

    for t in range(teams):
        feed(t, t <= team)

    def feed_later(t):
        @pl.when(team < t)
        def _():
            pl.semaphore_wait(ready_sem.at[t], 1)

        feed(t, team < t)

    for i in (4, 5):
        loads[i].wait()
    for h in range(heads):
        wide = slice(h * size, (h + 1) * size)
        cols = slice(h % per * size, (h % per + 1) * size)
        query = turned(iq_buf[:, wide].astype(jnp.float32), gain_buf[1])
        q_own[h // per, :, cols] = query.astype(jnp.bfloat16)
    for peer, mate in mates:
        q_copy(peer, mate, seat).start()
    kv_all[me] = kv_own[seat]
    q_team[seat] = q_own[seat]
    for t in range(1, last):
        feed_later(t)


    for i in range(6, 12):
        loads[i].wait()

    column = lax.broadcasted_iota(jnp.int32, (1, text_rows), 1)
    bias = jnp.where(column < length_buf[0], 0.0, LOW)

    def scores_of(query, key):
        return (
            lax.dot_general(
                query, key, (((1,), (1,)), ((), ())), preferred_element_type=jnp.float32
            )
            * scale
        )

    def text_part(h, rows, query):
        cols = slice(h * size, (h + 1) * size)
        count = query.shape[0]
        scores = scores_of(query, tk_buf[:, cols]) + bias
        top = jnp.max(scores, axis=-1, keepdims=True)
        expo = jnp.exp2(scores - top)
        total = jnp.sum(expo, axis=-1, keepdims=True)
        m_buf[h, rows] = jnp.broadcast_to(top, (count, size))
        l_buf[h, rows] = jnp.broadcast_to(total, (count, size))
        o_buf[h, rows] = jnp.dot(
            expo.astype(jnp.bfloat16),
            tv_buf[:, cols],
            preferred_element_type=jnp.float32,
        )

    for h in range(per):
        cols = slice(h * size, (h + 1) * size)
        key = tk_buf[:, cols].astype(jnp.float32)
        tk_buf[:, cols] = (key * rsqrt_mean(key) * gain_buf[2]).astype(jnp.bfloat16)
        query = tq_buf[:, cols].astype(jnp.float32)
        query = (query * rsqrt_mean(query) * gain_buf[3]).astype(jnp.bfloat16)
        qs[h, :team_text] = query
        text_part(h, slice(0, team_text), query)

        if h == 0:
            feed_later(last)

    for peer, mate in mates:
        q_copy(me, mate, mate).wait_recv()
    for h in range(per):
        cols = slice(h * size, (h + 1) * size)
        query = q_team[:, :, cols].astype(jnp.float32)
        query = query.reshape(TEAM * own_rows, size).astype(jnp.bfloat16)
        qs[h, team_text:] = query
        text_part(h, slice(team_text, team_rows), query)

    for t in range(teams):
        for k in (0, 1, 2, 3):
            origin = t * TEAM + (seat ^ k)

            @pl.when(origin != me)
            def _():
                kv_copy(me, origin).wait_recv()

    def gathered(start, h):
        cols = slice(h * size, (h + 1) * size)
        whole = kv_all[:, start : start + own_rows, cols].astype(jnp.float32)
        return whole.reshape(devices * own_rows, size).astype(jnp.bfloat16)

    every = range(per)
    scores = [scores_of(qs[h], gathered(0, h)) for h in every]
    olds = [m_buf[h] for h in every]
    tops = [
        jnp.maximum(olds[h][:, :1], jnp.max(scores[h], axis=-1, keepdims=True))
        for h in every
    ]
    expos = [jnp.exp2(scores[h] - tops[h]) for h in every]
    added = [
        jnp.dot(
            expos[h].astype(jnp.bfloat16),
            gathered(own_rows, h),
            preferred_element_type=jnp.float32,
        )
        for h in every
    ]
    sums = [jnp.sum(expos[h], axis=-1, keepdims=True) for h in every]
    for h in every:
        cols = slice(h * size, (h + 1) * size)
        back = jnp.exp2(olds[h] - tops[h])
        out = (o_buf[h] * back + added[h]) / (l_buf[h] * back + sums[h])
        for s in range(TEAM):
            part = jnp.concatenate(
                [
                    out[s * share : (s + 1) * share],
                    out[team_text + s * own_rows : team_text + (s + 1) * own_rows],
                ],
                axis=0,
            )
            back_own[s, :, cols] = part.astype(jnp.bfloat16)
    for mate in range(TEAM):

        @pl.when(mate != seat)
        def _():
            back_copy(team * TEAM + mate, mate, seat).start()

    back_all[seat] = back_own[seat]
    for d in range(1, devices):
        kv_copy((me + d) % devices, me).wait_send()
    for peer, mate in mates:
        q_copy(peer, mate, seat).wait_send()
    for peer, mate in mates:
        back_copy(me, mate, mate).wait_recv()
    out_ref[...] = back_all[...]

    for peer, mate in mates:
        back_copy(peer, mate, seat).wait_send()


def spread(parts_ref, io_ref, to_ref):
    share = to_ref.shape[0]
    span = parts_ref.shape[-1]
    for s in range(TEAM):
        cols = slice(s * span, (s + 1) * span)
        to_ref[:, cols] = parts_ref[s, :share]
        io_ref[:, cols] = parts_ref[s, share:]


def local(iq, ik, iv, tq, tk, tv, iqg, ikg, tqg, tkg, order, length):
    devices = lax.axis_size("seq")
    own_rows, width = iq.shape
    size = iqg.shape[0]
    span = width // TEAM
    per = span // size
    text_rows = tq.shape[0]
    share = text_rows // devices
    team_text = share * TEAM
    team_rows = team_text + TEAM * own_rows
    teams = devices // TEAM
    vmem = pl.BlockSpec(memory_space=pltpu.VMEM)
    hbm = pl.BlockSpec(memory_space=pl.ANY)
    gains = [g.reshape(1, size) for g in (iqg, ikg, tqg, tkg)]
    bf16, f32 = jnp.bfloat16, jnp.float32
    parts = pl.pallas_call(
        functools.partial(kernel, devices),
        out_shape=pltpu.VMEM((TEAM, share + own_rows, span), bf16),
        in_specs=[hbm] * 12,
        out_specs=vmem,
        scratch_shapes=[
            pltpu.VMEM((own_rows, width), bf16),
            pltpu.VMEM((own_rows, width), bf16),
            pltpu.VMEM((own_rows, width), bf16),
            pltpu.VMEM((team_text, span), bf16),
            pltpu.VMEM((text_rows, span), bf16),
            pltpu.VMEM((text_rows, span), bf16),
            pltpu.VMEM((4, 1, size), f32),
            pltpu.SMEM((own_rows,), jnp.int32),
            pltpu.SMEM((1,), jnp.int32),
            pltpu.VMEM((TEAM, 2 * own_rows, span), bf16),
            pltpu.VMEM((TEAM, own_rows, span), bf16),
            pltpu.VMEM((devices, 2 * own_rows, span), bf16),
            pltpu.VMEM((TEAM, own_rows, span), bf16),
            pltpu.VMEM((per, team_rows, size), bf16),
            pltpu.VMEM((per, team_rows, size), f32),
            pltpu.VMEM((per, team_rows, size), f32),
            pltpu.VMEM((per, team_rows, size), f32),
            pltpu.VMEM((TEAM, share + own_rows, span), bf16),
            pltpu.VMEM((TEAM, share + own_rows, span), bf16),
            pltpu.SemaphoreType.DMA((12,)),
            pltpu.SemaphoreType.DMA((devices,)),
            pltpu.SemaphoreType.DMA((devices,)),
            pltpu.SemaphoreType.REGULAR((teams,)),
            pltpu.SemaphoreType.DMA((TEAM,)),
            pltpu.SemaphoreType.DMA((TEAM,)),
            pltpu.SemaphoreType.DMA((TEAM,)),
            pltpu.SemaphoreType.DMA((TEAM,)),
        ],
        compiler_params=pltpu.CompilerParams(
            collective_id=0, has_side_effects=True, vmem_limit_bytes=62 * 1024 * 1024
        ),
    )(iq, ik, iv, tq, tk, tv, *gains, order, length)
    parts = pltpu.with_memory_space_constraint(parts, pltpu.VMEM)
    return pl.pallas_call(
        spread,
        out_shape=(
            jax.ShapeDtypeStruct((own_rows, width), bf16),
            jax.ShapeDtypeStruct((share, width), bf16),
        ),
        in_specs=[vmem],
        out_specs=(vmem, vmem),
    )(parts)


def solution(mesh):
    rows = P(("req", "seq"), None)
    text = P("req", None)
    return jax.shard_map(
        local,
        mesh=mesh,
        in_specs=(rows, rows, rows, text, text, text)
        + (P(), P(), P(), P(), P(("req", "seq")), P("req")),
        out_specs=(rows, rows),
        check_vma=False,
    )
```

```python
import functools
import math

import jax
import jax.numpy as jnp
from jax import lax
from jax.experimental import pallas as pl
from jax.experimental.pallas import tpu as pltpu
from jax.sharding import PartitionSpec as P

GRID_W = 64
EPS = 1e-06
LOW = -1e30
TEAM = 4
MAKERS = 3
ORDERS = ((2, 1, 0), (2, 1, 0), (1, 2, 0), (1, 2, 0))
MESH = pl.DeviceIdType.MESH


def rsqrt_mean(values):
    return lax.rsqrt(jnp.mean(values * values, axis=-1, keepdims=True) + EPS)


def kernel(
    devices,
    iq_ref,
    ik_ref,
    iv_ref,
    tq_ref,
    tk_ref,
    tv_ref,
    iqg_ref,
    ikg_ref,
    tqg_ref,
    tkg_ref,
    order_ref,
    length_ref,
    image_out_ref,
    text_out_ref,
    iq_buf,
    ik_buf,
    iv_buf,
    tq_buf,
    tk_buf,
    tv_buf,
    gain_buf,
    order_buf,
    length_buf,
    kv_own,
    q_own,
    kv_all,
    q_team,
    qs,
    m_buf,
    l_buf,
    o_buf,
    back_own,
    back_all,
    local_sem,
    kv_send,
    kv_recv,
    ready_sem,
    q_send,
    q_recv,
    back_send,
    back_recv,
):
    me = lax.axis_index("seq")
    req = lax.axis_index("req")
    seat = me % TEAM
    team = me // TEAM

    barrier = pltpu.get_barrier_semaphore()
    teams = devices // TEAM
    last = teams - 1
    for t in reversed(range(teams)):
        for k in (3, 2, 1, 0):
            peer = t * TEAM + (seat ^ k)

            @pl.when((peer != me) & (t >= team))
            def _():
                pl.semaphore_signal(
                    barrier, inc=1, device_id=(req, peer), device_id_type=MESH
                )

    own_rows, width = iq_buf.shape
    size = gain_buf.shape[-1]
    heads = width // size
    text_rows, span = tk_buf.shape
    per = span // size
    team_text = tq_buf.shape[0]
    share = team_text // TEAM
    team_rows = team_text + TEAM * own_rows
    scale = math.log2(math.e) / math.sqrt(size)

    makes = seat < MAKERS
    part = jnp.minimum(seat, MAKERS - 1)
    lanes = pl.ds(pl.multiple_of(part * span, span), span)
    text = pl.ds(pl.multiple_of(team * team_text, team_text), team_text)
    loads = []
    for src, dst in (
        (order_ref, order_buf),
        (ik_ref, ik_buf),
        (ikg_ref, gain_buf.at[0]),
        (iv_ref, iv_buf),
        (iq_ref, iq_buf),
        (iqg_ref, gain_buf.at[1]),
        (tk_ref.at[:, lanes], tk_buf),
        (tkg_ref, gain_buf.at[2]),
        (tq_ref.at[text, lanes], tq_buf),
        (tqg_ref, gain_buf.at[3]),
        (length_ref, length_buf),
        (tv_ref.at[:, lanes], tv_buf),
    ):
        copy = pltpu.make_async_copy(src, dst, local_sem.at[len(loads)])
        copy.start()
        loads.append(copy)

    loads[0].wait()
    half_length = own_rows * devices // 2
    lane = lax.broadcasted_iota(jnp.int32, (own_rows, size), 1)
    row = lax.broadcasted_iota(jnp.int32, (own_rows, size), 0)
    pair_id = lane // 2
    first = pair_id < 8
    second = pair_id < 36
    coordinate = jnp.zeros((own_rows, size), jnp.int32)
    for r in range(own_rows):
        position = order_buf[r]
        inside = position % half_length
        here = jnp.where(
            first,
            position // half_length,
            jnp.where(second, inside // GRID_W, inside % GRID_W),
        )
        coordinate = jnp.where(row == r, here, coordinate)
    within = jnp.where(first, pair_id, jnp.where(second, pair_id - 8, pair_id - 36))
    step = jnp.where(first, 2.0 / 16.0, 2.0 / 56.0) * (-math.log(10000.0))
    angle = coordinate.astype(jnp.float32) * jnp.exp(within.astype(jnp.float32) * step)
    cosine = jnp.cos(angle)
    sine = jnp.sin(angle)
    even = lane % 2 == 0
    sine = jnp.where(even, -sine, sine)

    def turned(values, gain):
        normed = values * rsqrt_mean(values) * gain
        swapped = jnp.where(
            even, pltpu.roll(normed, size - 1, 1), pltpu.roll(normed, 1, 1)
        )
        return normed * cosine + swapped * sine

    for i in (1, 2, 3):
        loads[i].wait()
    for h in range(heads):
        wide = slice(h * size, (h + 1) * size)
        cols = slice(h % per * size, (h % per + 1) * size)
        key = turned(ik_buf[:, wide].astype(jnp.float32), gain_buf[0])
        both = jnp.concatenate([key, iv_buf[:, wide].astype(jnp.float32)], axis=0)
        kv_own[h // per, :, cols] = both.astype(jnp.bfloat16)

    pl.semaphore_wait(barrier, (team + 1) * TEAM - 1)

    def remote(src, dst, send, recv, peer):
        return pltpu.make_async_remote_copy(
            src_ref=src,
            dst_ref=dst,
            send_sem=send,
            recv_sem=recv,
            device_id=(req, peer),
            device_id_type=MESH,
        )

    def kv_copy(peer, origin):
        return remote(
            kv_own.at[peer % TEAM],
            kv_all.at[origin],
            kv_send.at[peer],
            kv_recv.at[origin],
            peer,
        )

    def q_copy(mate):
        return remote(
            q_own.at[mate],
            q_team.at[seat],
            q_send.at[mate],
            q_recv.at[seat],
            team * TEAM + mate,
        )

    def back_copy(mate):
        return remote(
            back_own.at[mate],
            back_all.at[part],
            back_send.at[mate],
            back_recv.at[part],
            team * TEAM + mate,
        )

    def arrive(buf, sends, arrivals, origin):
        here = buf.at[origin]
        remote(here, here, sends.at[0], arrivals.at[origin], me).wait_recv()

    for t in range(last):

        @pl.when(t < team)
        def _():
            pl.semaphore_signal(
                ready_sem.at[team],
                inc=1,
                device_id=(req, t * TEAM + seat),
                device_id_type=MESH,
            )

    def pick(values):
        value = values[-1]
        for place in reversed(range(TEAM - 1)):
            value = jnp.where(seat == place, values[place], value)
        return value

    places = [pick(column) for column in zip(*ORDERS)]

    def feed(t, allowed):
        for place in places:
            peer = t * TEAM + place

            @pl.when((peer != me) & allowed)
            def _():
                kv_copy(peer, me).start()

    for t in range(teams):
        feed(t, t <= team)

    def feed_later(t):
        @pl.when(team < t)
        def _():
            pl.semaphore_wait(ready_sem.at[t], 1)

        feed(t, team < t)

    for i in (4, 5):
        loads[i].wait()
    for h in range(heads):
        wide = slice(h * size, (h + 1) * size)
        cols = slice(h % per * size, (h % per + 1) * size)
        query = turned(iq_buf[:, wide].astype(jnp.float32), gain_buf[1])
        q_own[h // per, :, cols] = query.astype(jnp.bfloat16)
    for mate in reversed(range(MAKERS)):

        @pl.when(mate != seat)
        def _():
            q_copy(mate).start()

    kv_all[me] = kv_own[part]
    q_team[seat] = q_own[part]
    for t in range(1, teams):
        feed_later(t)


    for i in range(6, 12):
        loads[i].wait()

    column = lax.broadcasted_iota(jnp.int32, (1, text_rows), 1)
    bias = jnp.where(column < length_buf[0], 0.0, LOW)

    def scores_of(query, key):
        return (
            lax.dot_general(
                query, key, (((1,), (1,)), ((), ())), preferred_element_type=jnp.float32
            )
            * scale
        )

    def text_part(h, rows, query):
        cols = slice(h * size, (h + 1) * size)
        count = query.shape[0]
        scores = scores_of(query, tk_buf[:, cols]) + bias
        top = jnp.max(scores, axis=-1, keepdims=True)
        expo = jnp.exp2(scores - top)
        total = jnp.sum(expo, axis=-1, keepdims=True)
        m_buf[h, rows] = jnp.broadcast_to(top, (count, size))
        l_buf[h, rows] = jnp.broadcast_to(total, (count, size))
        o_buf[h, rows] = jnp.dot(
            expo.astype(jnp.bfloat16),
            tv_buf[:, cols],
            preferred_element_type=jnp.float32,
        )

    def gathered(start, h):
        cols = slice(h * size, (h + 1) * size)
        whole = kv_all[:, start : start + own_rows, cols]
        return whole.reshape(devices * own_rows, size)

    @pl.when(makes)
    def _():
        for h in range(per):
            cols = slice(h * size, (h + 1) * size)
            key = tk_buf[:, cols].astype(jnp.float32)
            tk_buf[:, cols] = (key * rsqrt_mean(key) * gain_buf[2]).astype(jnp.bfloat16)
            query = tq_buf[:, cols].astype(jnp.float32)
            query = (query * rsqrt_mean(query) * gain_buf[3]).astype(jnp.bfloat16)
            qs[h, :team_text] = query
            text_part(h, slice(0, team_text), query)

        for k in (3, 2, 1):
            arrive(q_team, q_send, q_recv, seat ^ k)
        for h in range(per):
            cols = slice(h * size, (h + 1) * size)
            query = q_team[:, :, cols].astype(jnp.float32)
            query = query.reshape(TEAM * own_rows, size).astype(jnp.bfloat16)
            qs[h, team_text:] = query
            text_part(h, slice(team_text, team_rows), query)

        for t in range(teams):
            for k in (0, 1, 2, 3):
                origin = t * TEAM + (seat ^ k)

                @pl.when(origin != me)
                def _():
                    arrive(kv_all, kv_send, kv_recv, origin)

        every = range(per)
        scores = [scores_of(qs[h], gathered(0, h)) for h in every]
        olds = [m_buf[h] for h in every]
        tops = [
            jnp.maximum(olds[h][:, :1], jnp.max(scores[h], axis=-1, keepdims=True))
            for h in every
        ]
        expos = [jnp.exp2(scores[h] - tops[h]) for h in every]
        added = [
            jnp.dot(
                expos[h].astype(jnp.bfloat16),
                gathered(own_rows, h),
                preferred_element_type=jnp.float32,
            )
            for h in every
        ]
        sums = [jnp.sum(expos[h], axis=-1, keepdims=True) for h in every]
        for h in every:
            cols = slice(h * size, (h + 1) * size)
            back = jnp.exp2(olds[h] - tops[h])
            out = (o_buf[h] * back + added[h]) / (l_buf[h] * back + sums[h])
            for s in range(TEAM):
                rows = jnp.concatenate(
                    [
                        out[s * share : (s + 1) * share],
                        out[team_text + s * own_rows : team_text + (s + 1) * own_rows],
                    ],
                    axis=0,
                )
                back_own[s, :, cols] = rows.astype(jnp.bfloat16)
        for mate in range(TEAM):

            @pl.when(mate != seat)
            def _():
                back_copy(mate).start()

        back_all[seat] = back_own[seat]

    for t in range(teams):
        for place in range(MAKERS):
            peer = t * TEAM + place

            @pl.when(peer != me)
            def _():
                kv_copy(peer, me).wait_send()

    for mate in range(MAKERS):

        @pl.when(mate != seat)
        def _():
            q_copy(mate).wait_send()

    for origin in reversed(range(MAKERS)):

        @pl.when(origin != seat)
        def _():
            arrive(back_all, back_send, back_recv, origin)

    for place in range(MAKERS):
        cols = slice(place * span, (place + 1) * span)
        text_out_ref[:, cols] = back_all[place, :share]
        image_out_ref[:, cols] = back_all[place, share:]

    for mate in range(TEAM):

        @pl.when(makes & (mate != seat))
        def _():
            back_copy(mate).wait_send()


def store(image_ref, text_ref, io_ref, to_ref, sems):
    copies = [
        pltpu.make_async_copy(image_ref, io_ref, sems.at[0]),
        pltpu.make_async_copy(text_ref, to_ref, sems.at[1]),
    ]
    for copy in copies:
        copy.start()
    for copy in copies:
        copy.wait()


def local(iq, ik, iv, tq, tk, tv, iqg, ikg, tqg, tkg, order, length):
    devices = lax.axis_size("seq")
    own_rows, width = iq.shape
    size = iqg.shape[0]
    span = width // MAKERS
    per = span // size
    text_rows = tq.shape[0]
    share = text_rows // devices
    team_text = share * TEAM
    team_rows = team_text + TEAM * own_rows
    teams = devices // TEAM
    vmem = pl.BlockSpec(memory_space=pltpu.VMEM)
    hbm = pl.BlockSpec(memory_space=pl.ANY)
    gains = [g.reshape(1, size) for g in (iqg, ikg, tqg, tkg)]
    bf16, f32 = jnp.bfloat16, jnp.float32
    parts = pl.pallas_call(
        functools.partial(kernel, devices),
        out_shape=(
            pltpu.VMEM((own_rows, width), bf16),
            pltpu.VMEM((share, width), bf16),
        ),
        in_specs=[hbm] * 12,
        out_specs=(vmem, vmem),
        scratch_shapes=[
            pltpu.VMEM((own_rows, width), bf16),
            pltpu.VMEM((own_rows, width), bf16),
            pltpu.VMEM((own_rows, width), bf16),
            pltpu.VMEM((team_text, span), bf16),
            pltpu.VMEM((text_rows, span), bf16),
            pltpu.VMEM((text_rows, span), bf16),
            pltpu.VMEM((4, 1, size), f32),
            pltpu.SMEM((own_rows,), jnp.int32),
            pltpu.SMEM((1,), jnp.int32),
            pltpu.VMEM((MAKERS, 2 * own_rows, span), bf16),
            pltpu.VMEM((MAKERS, own_rows, span), bf16),
            pltpu.VMEM((devices, 2 * own_rows, span), bf16),
            pltpu.VMEM((TEAM, own_rows, span), bf16),
            pltpu.VMEM((per, team_rows, size), bf16),
            pltpu.VMEM((per, team_rows, size), f32),
            pltpu.VMEM((per, team_rows, size), f32),
            pltpu.VMEM((per, team_rows, size), f32),
            pltpu.VMEM((TEAM, share + own_rows, span), bf16),
            pltpu.VMEM((MAKERS, share + own_rows, span), bf16),
            pltpu.SemaphoreType.DMA((12,)),
            pltpu.SemaphoreType.DMA((devices,)),
            pltpu.SemaphoreType.DMA((devices,)),
            pltpu.SemaphoreType.REGULAR((teams,)),
            pltpu.SemaphoreType.DMA((TEAM,)),
            pltpu.SemaphoreType.DMA((TEAM,)),
            pltpu.SemaphoreType.DMA((TEAM,)),
            pltpu.SemaphoreType.DMA((TEAM,)),
        ],
        compiler_params=pltpu.CompilerParams(
            collective_id=0, has_side_effects=True, vmem_limit_bytes=62 * 1024 * 1024
        ),
    )(iq, ik, iv, tq, tk, tv, *gains, order, length)
    parts = [pltpu.with_memory_space_constraint(p, pltpu.VMEM) for p in parts]
    return pl.pallas_call(
        store,
        out_shape=(
            jax.ShapeDtypeStruct((own_rows, width), bf16),
            jax.ShapeDtypeStruct((share, width), bf16),
        ),
        in_specs=[vmem, vmem],
        out_specs=(hbm, hbm),
        scratch_shapes=[pltpu.SemaphoreType.DMA((2,))],
    )(*parts)


def solution(mesh):
    rows = P(("req", "seq"), None)
    text = P("req", None)
    return jax.shard_map(
        local,
        mesh=mesh,
        in_specs=(rows, rows, rows, text, text, text)
        + (P(), P(), P(), P(), P(("req", "seq")), P("req")),
        out_specs=(rows, rows),
        check_vma=False,
    )
```

```python
import functools
import math

import jax
import jax.numpy as jnp
from jax import lax
from jax.experimental import pallas as pl
from jax.experimental.pallas import tpu as pltpu
from jax.sharding import PartitionSpec as P

GRID_W = 64
EPS = 1e-06
LOW = -1e30
TEAM = 4
MAKERS = 3
ORDERS = ((2, 1, 0), (2, 1, 0), (1, 2, 0), (1, 2, 0))
MESH = pl.DeviceIdType.MESH


def rsqrt_mean(values):
    return lax.rsqrt(jnp.mean(values * values, axis=-1, keepdims=True) + EPS)


def kernel(
    devices,
    iq_ref,
    ik_ref,
    iv_ref,
    tq_ref,
    tk_ref,
    tv_ref,
    iqg_ref,
    ikg_ref,
    tqg_ref,
    tkg_ref,
    order_ref,
    length_ref,
    image_out_ref,
    text_out_ref,
    iq_buf,
    ik_buf,
    iv_buf,
    tq_buf,
    tk_buf,
    tv_buf,
    gain_buf,
    order_buf,
    length_buf,
    kv_own,
    q_own,
    kv_all,
    q_team,
    qs,
    m_buf,
    l_buf,
    o_buf,
    back_own,
    back_all,
    local_sem,
    kv_send,
    kv_recv,
    ready_sem,
    q_send,
    q_recv,
    back_send,
    back_recv,
):
    me = lax.axis_index("seq")
    req = lax.axis_index("req")
    seat = me % TEAM
    team = me // TEAM

    barrier = pltpu.get_barrier_semaphore()
    teams = devices // TEAM
    last = teams - 1
    for t in reversed(range(teams)):
        for k in (3, 2, 1, 0):
            peer = t * TEAM + (seat ^ k)

            @pl.when((peer != me) & (t >= team))
            def _():
                pl.semaphore_signal(
                    barrier, inc=1, device_id=(req, peer), device_id_type=MESH
                )

    own_rows, width = iq_buf.shape
    size = gain_buf.shape[-1]
    heads = width // size
    text_rows, span = tk_buf.shape
    per = span // size
    team_text = tq_buf.shape[0]
    share = team_text // TEAM
    team_rows = team_text + TEAM * own_rows
    scale = math.log2(math.e) / math.sqrt(size)

    makes = seat < MAKERS
    part = jnp.minimum(seat, MAKERS - 1)
    lanes = pl.ds(pl.multiple_of(part * span, span), span)
    text = pl.ds(pl.multiple_of(team * team_text, team_text), team_text)
    loads = []
    for src, dst in (
        (order_ref, order_buf),
        (ik_ref, ik_buf),
        (ikg_ref, gain_buf.at[0]),
        (iv_ref, iv_buf),
        (iq_ref, iq_buf),
        (iqg_ref, gain_buf.at[1]),
        (tk_ref.at[:, lanes], tk_buf),
        (tkg_ref, gain_buf.at[2]),
        (tq_ref.at[text, lanes], tq_buf),
        (tqg_ref, gain_buf.at[3]),
        (length_ref, length_buf),
        (tv_ref.at[:, lanes], tv_buf),
    ):
        copy = pltpu.make_async_copy(src, dst, local_sem.at[len(loads)])
        copy.start()
        loads.append(copy)

    loads[0].wait()
    half_length = own_rows * devices // 2
    lane = lax.broadcasted_iota(jnp.int32, (own_rows, size), 1)
    row = lax.broadcasted_iota(jnp.int32, (own_rows, size), 0)
    pair_id = lane // 2
    first = pair_id < 8
    second = pair_id < 36
    coordinate = jnp.zeros((own_rows, size), jnp.int32)
    for r in range(own_rows):
        position = order_buf[r]
        inside = position % half_length
        here = jnp.where(
            first,
            position // half_length,
            jnp.where(second, inside // GRID_W, inside % GRID_W),
        )
        coordinate = jnp.where(row == r, here, coordinate)
    within = jnp.where(first, pair_id, jnp.where(second, pair_id - 8, pair_id - 36))
    step = jnp.where(first, 2.0 / 16.0, 2.0 / 56.0) * (-math.log(10000.0))
    angle = coordinate.astype(jnp.float32) * jnp.exp(within.astype(jnp.float32) * step)
    cosine = jnp.cos(angle)
    sine = jnp.sin(angle)
    even = lane % 2 == 0
    sine = jnp.where(even, -sine, sine)

    def turned(values, gain):
        normed = values * rsqrt_mean(values) * gain
        swapped = jnp.where(
            even, pltpu.roll(normed, size - 1, 1), pltpu.roll(normed, 1, 1)
        )
        return normed * cosine + swapped * sine

    for i in (1, 2, 3):
        loads[i].wait()
    for h in range(heads):
        wide = slice(h * size, (h + 1) * size)
        cols = slice(h % per * size, (h % per + 1) * size)
        key = turned(ik_buf[:, wide].astype(jnp.float32), gain_buf[0])
        both = jnp.concatenate([key, iv_buf[:, wide].astype(jnp.float32)], axis=0)
        kv_own[h // per, :, cols] = both.astype(jnp.bfloat16)

    pl.semaphore_wait(barrier, (team + 1) * TEAM - 1)

    def remote(src, dst, send, recv, peer):
        return pltpu.make_async_remote_copy(
            src_ref=src,
            dst_ref=dst,
            send_sem=send,
            recv_sem=recv,
            device_id=(req, peer),
            device_id_type=MESH,
        )

    def kv_copy(peer, origin):
        return remote(
            kv_own.at[peer % TEAM],
            kv_all.at[origin],
            kv_send.at[peer],
            kv_recv.at[origin],
            peer,
        )

    def q_copy(mate):
        return remote(
            q_own.at[mate],
            q_team.at[seat],
            q_send.at[mate],
            q_recv.at[seat],
            team * TEAM + mate,
        )

    def back_copy(mate):
        return remote(
            back_own.at[mate],
            back_all.at[part],
            back_send.at[mate],
            back_recv.at[part],
            team * TEAM + mate,
        )

    def arrive(buf, sends, arrivals, origin):
        here = buf.at[origin]
        remote(here, here, sends.at[0], arrivals.at[origin], me).wait_recv()

    for t in range(last):

        @pl.when(t < team)
        def _():
            pl.semaphore_signal(
                ready_sem.at[team],
                inc=1,
                device_id=(req, t * TEAM + seat),
                device_id_type=MESH,
            )

    def pick(values):
        value = values[-1]
        for place in reversed(range(TEAM - 1)):
            value = jnp.where(seat == place, values[place], value)
        return value

    places = [pick(column) for column in zip(*ORDERS)]

    def feed(t, allowed):
        for place in places:
            peer = t * TEAM + place

            @pl.when((peer != me) & allowed)
            def _():
                kv_copy(peer, me).start()

    feed(0, True)

    def feed_later(t):
        @pl.when(team < t)
        def _():
            pl.semaphore_wait(ready_sem.at[t], 1)

        feed(t, team < t)

    for i in (4, 5):
        loads[i].wait()
    for h in range(heads):
        wide = slice(h * size, (h + 1) * size)
        cols = slice(h % per * size, (h % per + 1) * size)
        query = turned(iq_buf[:, wide].astype(jnp.float32), gain_buf[1])
        q_own[h // per, :, cols] = query.astype(jnp.bfloat16)
    for mate in reversed(range(MAKERS)):

        @pl.when(mate != seat)
        def _():
            q_copy(mate).start()

    kv_all[me] = kv_own[part]
    q_team[seat] = q_own[part]
    for t in range(1, teams):
        feed(t, t <= team)
    for t in range(1, teams):
        feed_later(t)


    for i in range(6, 12):
        loads[i].wait()

    column = lax.broadcasted_iota(jnp.int32, (1, text_rows), 1)
    bias = jnp.where(column < length_buf[0], 0.0, LOW)

    def scores_of(query, key):
        return (
            lax.dot_general(
                query, key, (((1,), (1,)), ((), ())), preferred_element_type=jnp.float32
            )
            * scale
        )

    def text_part(h, rows, query):
        cols = slice(h * size, (h + 1) * size)
        count = query.shape[0]
        scores = scores_of(query, tk_buf[:, cols]) + bias
        top = jnp.max(scores, axis=-1, keepdims=True)
        expo = jnp.exp2(scores - top)
        total = jnp.sum(expo, axis=-1, keepdims=True)
        m_buf[h, rows] = jnp.broadcast_to(top, (count, size))
        l_buf[h, rows] = jnp.broadcast_to(total, (count, size))
        o_buf[h, rows] = jnp.dot(
            expo.astype(jnp.bfloat16),
            tv_buf[:, cols],
            preferred_element_type=jnp.float32,
        )

    def gathered(start, h):
        cols = slice(h * size, (h + 1) * size)
        whole = kv_all[:, start : start + own_rows, cols]
        return whole.reshape(devices * own_rows, size)

    @pl.when(makes)
    def _():
        for h in range(per):
            cols = slice(h * size, (h + 1) * size)
            key = tk_buf[:, cols].astype(jnp.float32)
            tk_buf[:, cols] = (key * rsqrt_mean(key) * gain_buf[2]).astype(jnp.bfloat16)
            query = tq_buf[:, cols].astype(jnp.float32)
            query = (query * rsqrt_mean(query) * gain_buf[3]).astype(jnp.bfloat16)
            qs[h, :team_text] = query
            text_part(h, slice(0, team_text), query)

        for k in (3, 2, 1):
            arrive(q_team, q_send, q_recv, seat ^ k)
        for h in range(per):
            cols = slice(h * size, (h + 1) * size)
            query = q_team[:, :, cols].astype(jnp.float32)
            query = query.reshape(TEAM * own_rows, size).astype(jnp.bfloat16)
            qs[h, team_text:] = query
            text_part(h, slice(team_text, team_rows), query)

        for t in range(teams):
            for k in (0, 1, 2, 3):
                origin = t * TEAM + (seat ^ k)

                @pl.when(origin != me)
                def _():
                    arrive(kv_all, kv_send, kv_recv, origin)

        every = range(per)
        scores = [scores_of(qs[h], gathered(0, h)) for h in every]
        olds = [m_buf[h] for h in every]
        tops = [
            jnp.maximum(olds[h][:, :1], jnp.max(scores[h], axis=-1, keepdims=True))
            for h in every
        ]
        expos = [jnp.exp2(scores[h] - tops[h]) for h in every]
        added = [
            jnp.dot(
                expos[h].astype(jnp.bfloat16),
                gathered(own_rows, h),
                preferred_element_type=jnp.float32,
            )
            for h in every
        ]
        sums = [jnp.sum(expos[h], axis=-1, keepdims=True) for h in every]
        for h in every:
            cols = slice(h * size, (h + 1) * size)
            back = jnp.exp2(olds[h] - tops[h])
            out = (o_buf[h] * back + added[h]) / (l_buf[h] * back + sums[h])
            for s in range(TEAM):
                rows = jnp.concatenate(
                    [
                        out[s * share : (s + 1) * share],
                        out[team_text + s * own_rows : team_text + (s + 1) * own_rows],
                    ],
                    axis=0,
                )
                back_own[s, :, cols] = rows.astype(jnp.bfloat16)
        for mate in range(TEAM):

            @pl.when(mate != seat)
            def _():
                back_copy(mate).start()

        back_all[seat] = back_own[seat]

    for t in range(teams):
        for place in range(MAKERS):
            peer = t * TEAM + place

            @pl.when(peer != me)
            def _():
                kv_copy(peer, me).wait_send()

    for mate in range(MAKERS):

        @pl.when(mate != seat)
        def _():
            q_copy(mate).wait_send()

    for origin in reversed(range(MAKERS)):

        @pl.when(origin != seat)
        def _():
            arrive(back_all, back_send, back_recv, origin)

    for place in range(MAKERS):
        cols = slice(place * span, (place + 1) * span)
        text_out_ref[:, cols] = back_all[place, :share]
        image_out_ref[:, cols] = back_all[place, share:]

    for mate in range(TEAM):

        @pl.when(makes & (mate != seat))
        def _():
            back_copy(mate).wait_send()


def store(image_ref, text_ref, io_ref, to_ref, sems):
    copies = [
        pltpu.make_async_copy(image_ref, io_ref, sems.at[0]),
        pltpu.make_async_copy(text_ref, to_ref, sems.at[1]),
    ]
    for copy in copies:
        copy.start()
    for copy in copies:
        copy.wait()


def local(iq, ik, iv, tq, tk, tv, iqg, ikg, tqg, tkg, order, length):
    devices = lax.axis_size("seq")
    own_rows, width = iq.shape
    size = iqg.shape[0]
    span = width // MAKERS
    per = span // size
    text_rows = tq.shape[0]
    share = text_rows // devices
    team_text = share * TEAM
    team_rows = team_text + TEAM * own_rows
    teams = devices // TEAM
    vmem = pl.BlockSpec(memory_space=pltpu.VMEM)
    hbm = pl.BlockSpec(memory_space=pl.ANY)
    gains = [g.reshape(1, size) for g in (iqg, ikg, tqg, tkg)]
    bf16, f32 = jnp.bfloat16, jnp.float32
    parts = pl.pallas_call(
        functools.partial(kernel, devices),
        out_shape=(
            pltpu.VMEM((own_rows, width), bf16),
            pltpu.VMEM((share, width), bf16),
        ),
        in_specs=[hbm] * 12,
        out_specs=(vmem, vmem),
        scratch_shapes=[
            pltpu.VMEM((own_rows, width), bf16),
            pltpu.VMEM((own_rows, width), bf16),
            pltpu.VMEM((own_rows, width), bf16),
            pltpu.VMEM((team_text, span), bf16),
            pltpu.VMEM((text_rows, span), bf16),
            pltpu.VMEM((text_rows, span), bf16),
            pltpu.VMEM((4, 1, size), f32),
            pltpu.SMEM((own_rows,), jnp.int32),
            pltpu.SMEM((1,), jnp.int32),
            pltpu.VMEM((MAKERS, 2 * own_rows, span), bf16),
            pltpu.VMEM((MAKERS, own_rows, span), bf16),
            pltpu.VMEM((devices, 2 * own_rows, span), bf16),
            pltpu.VMEM((TEAM, own_rows, span), bf16),
            pltpu.VMEM((per, team_rows, size), bf16),
            pltpu.VMEM((per, team_rows, size), f32),
            pltpu.VMEM((per, team_rows, size), f32),
            pltpu.VMEM((per, team_rows, size), f32),
            pltpu.VMEM((TEAM, share + own_rows, span), bf16),
            pltpu.VMEM((MAKERS, share + own_rows, span), bf16),
            pltpu.SemaphoreType.DMA((12,)),
            pltpu.SemaphoreType.DMA((devices,)),
            pltpu.SemaphoreType.DMA((devices,)),
            pltpu.SemaphoreType.REGULAR((teams,)),
            pltpu.SemaphoreType.DMA((TEAM,)),
            pltpu.SemaphoreType.DMA((TEAM,)),
            pltpu.SemaphoreType.DMA((TEAM,)),
            pltpu.SemaphoreType.DMA((TEAM,)),
        ],
        compiler_params=pltpu.CompilerParams(
            collective_id=0, has_side_effects=True, vmem_limit_bytes=62 * 1024 * 1024
        ),
    )(iq, ik, iv, tq, tk, tv, *gains, order, length)
    parts = [pltpu.with_memory_space_constraint(p, pltpu.VMEM) for p in parts]
    return pl.pallas_call(
        store,
        out_shape=(
            jax.ShapeDtypeStruct((own_rows, width), bf16),
            jax.ShapeDtypeStruct((share, width), bf16),
        ),
        in_specs=[vmem, vmem],
        out_specs=(hbm, hbm),
        scratch_shapes=[pltpu.SemaphoreType.DMA((2,))],
    )(*parts)


def solution(mesh):
    rows = P(("req", "seq"), None)
    text = P("req", None)
    return jax.shard_map(
        local,
        mesh=mesh,
        in_specs=(rows, rows, rows, text, text, text)
        + (P(), P(), P(), P(), P(("req", "seq")), P("req")),
        out_specs=(rows, rows),
        check_vma=False,
    )
```
